32 devices in a mesh: dp: 4 (over y, z), tp: 8 (over x, core).
Axes of the slice: x: 4, y: 2, z: 2, core: 2. Of those that a mesh axis runs over, the one named last changes fastest.
The devices are a block of a 4x4x8 slice.
Arguments:
- hidden: bfloat16 [8, 1024, 4096], P('dp', 'tp'), parts along dimension 0
- positions: int32 [8, 1024], P('dp', 'tp'), parts along dimension 0
- doc_ids: int32 [8, 1024], P('dp', 'tp'), parts along dimension 0
- norm_gain: bfloat16 [4096], replicated
- w_query: bfloat16 [4096, 4096], P(None, 'tp')
- w_key: bfloat16 [4096, 4096], P(None, 'tp')
- w_value: bfloat16 [4096, 4096], P(None, 'tp')
- w_out: bfloat16 [4096, 4096], P('tp')
- grad_out: bfloat16 [8, 1024, 4096], P('dp', 'tp'), parts along dimension 0
Outputs:
- output 1: bfloat16 [8, 1024, 4096], P('dp', 'tp'), parts along dimension 0
- output 2: bfloat16 [8, 1024, 4096], P('dp', 'tp'), parts along dimension 0
- output 3: float32 [16384], P('dp'), parts along dimension 0
- output 4: float32 [16384, 4096], P('dp', 'tp'), parts along dimension 0
- output 5: float32 [16384, 4096], P('dp', 'tp'), parts along dimension 0
- output 6: float32 [16384, 4096], P('dp', 'tp'), parts along dimension 0
- output 7: float32 [16384, 4096], P(('dp', 'tp')), parts along dimension 0
There are 4 independent parts. The reference program is written for one: setup_inputs(seed, part) draws one part's arguments, and reference() takes and returns one part's arrays. A program takes and returns all parts, laid end to end along the dimension named above; an argument that names none is the same for every part.
All inputs are finite; a program needn't handle non-finite values.
Results may differ from the reference program's by a relative error of at most 0.00957696.
Values are sent between devices in bfloat16 or wider.
A program may use at most 768 MiB of HBM per device.

```python
import jax
import jax.numpy as jnp
from jax import lax

BATCH_ROWS = 2
SEQ_LEN = 1024
MODEL_DIM = 4096
NUM_HEADS = 32
NUM_KV_HEADS = 32
HEAD_DIM = 128
NORM_EPS = 1e-5
ROPE_BASE = 10000.0


def draw_documents(doc_key):
    doc_mean = max(4, SEQ_LEN // 8)
    token_idx = jnp.arange(SEQ_LEN, dtype=jnp.int32)
    starts = jax.random.randint(doc_key, (BATCH_ROWS, SEQ_LEN), 0, doc_mean) == 0
    starts = starts | (token_idx == 0)[None, :]
    doc_ids = jnp.cumsum(starts.astype(jnp.int32), axis=1) - 1
    begins = lax.cummax(jnp.where(starts, token_idx[None, :], 0), axis=1)
    return (token_idx[None, :] - begins).astype(jnp.int32), doc_ids.astype(jnp.int32)


def setup_inputs(seed: int = 0, part: int = 0) -> dict:
    part_key = jax.random.fold_in(jax.random.key(seed), part)
    shared_key = jax.random.key(seed + 1)
    k_hidden, k_grad, k_doc = jax.random.split(part_key, 3)
    k_gain, k_query, k_key, k_value, k_out = jax.random.split(shared_key, 5)
    positions, doc_ids = draw_documents(k_doc)
    in_scale = MODEL_DIM ** -0.5
    out_scale = 2.0 * (NUM_HEADS * HEAD_DIM) ** -0.5
    q_width = NUM_HEADS * HEAD_DIM
    kv_width = NUM_KV_HEADS * HEAD_DIM
    return {
        'hidden': jax.random.normal(k_hidden, (BATCH_ROWS, SEQ_LEN, MODEL_DIM), jnp.float32).astype(jnp.bfloat16),
        'positions': positions,
        'doc_ids': doc_ids,
        'norm_gain': (1.0 + 0.3 * jax.random.normal(k_gain, (MODEL_DIM,), jnp.float32)).astype(jnp.bfloat16),
        'w_query': (in_scale * jax.random.normal(k_query, (MODEL_DIM, q_width), jnp.float32)).astype(jnp.bfloat16),
        'w_key': (in_scale * jax.random.normal(k_key, (MODEL_DIM, kv_width), jnp.float32)).astype(jnp.bfloat16),
        'w_value': (in_scale * jax.random.normal(k_value, (MODEL_DIM, kv_width), jnp.float32)).astype(jnp.bfloat16),
        'w_out': (out_scale * jax.random.normal(k_out, (q_width, MODEL_DIM), jnp.float32)).astype(jnp.bfloat16),
        'grad_out': jax.random.normal(k_grad, (BATCH_ROWS, SEQ_LEN, MODEL_DIM), jnp.float32).astype(jnp.bfloat16),
    }


def snap_bf16(values):
    return values + lax.stop_gradient(values.astype(jnp.bfloat16).astype(values.dtype) - values)


def rotate_pairs(values, cos_tab, sin_tab):
    pair_view = values.reshape(values.shape[:-1] + (HEAD_DIM // 2, 2))
    even_part = pair_view[..., 0]
    odd_part = pair_view[..., 1]
    turned = jnp.stack([even_part * cos_tab - odd_part * sin_tab, even_part * sin_tab + odd_part * cos_tab], axis=-1)
    return turned.reshape(values.shape)


def reference(hidden, positions, doc_ids, norm_gain, w_query, w_key, w_value, w_out, grad_out):
    group_size = NUM_HEADS // NUM_KV_HEADS
    attn_scale = HEAD_DIM ** -0.5
    inv_freq = ROPE_BASE ** (-jnp.arange(0, HEAD_DIM, 2, dtype=jnp.float32) / HEAD_DIM)
    angles = positions.astype(jnp.float32)[:, :, None] * inv_freq
    cos_tab = jnp.cos(angles)[:, :, None, :]
    sin_tab = jnp.sin(angles)[:, :, None, :]
    token_idx = jnp.arange(SEQ_LEN, dtype=jnp.int32)
    allowed = (doc_ids[:, :, None] == doc_ids[:, None, :]) & (token_idx[None, :] <= token_idx[:, None])[None]

    def head_group(operands):
        query_grp, key_grp, value_grp = operands
        scores = jnp.einsum('bqgd,bkd->bgqk', query_grp, key_grp) * attn_scale
        scores = jnp.where(allowed[:, None], scores, -1e30)
        attn_probs = snap_bf16(jax.nn.softmax(scores, axis=-1))
        return snap_bf16(jnp.einsum('bgqk,bkd->bqgd', attn_probs, value_grp))

    def forward(hidden_f32, gain_f32, wq_f32, wk_f32, wv_f32, wo_f32):
        mean_sq = jnp.mean(hidden_f32 * hidden_f32, axis=-1, keepdims=True)
        normed = snap_bf16(hidden_f32 * lax.rsqrt(mean_sq + NORM_EPS) * gain_f32)
        query_raw = jnp.dot(normed, wq_f32).reshape(BATCH_ROWS, SEQ_LEN, NUM_HEADS, HEAD_DIM)
        key_raw = jnp.dot(normed, wk_f32).reshape(BATCH_ROWS, SEQ_LEN, NUM_KV_HEADS, HEAD_DIM)
        query_rot = snap_bf16(rotate_pairs(query_raw, cos_tab, sin_tab))
        key_rot = snap_bf16(rotate_pairs(key_raw, cos_tab, sin_tab))
        value_rows = snap_bf16(jnp.dot(normed, wv_f32)).reshape(BATCH_ROWS, SEQ_LEN, NUM_KV_HEADS, HEAD_DIM)
        query_groups = jnp.moveaxis(query_rot.reshape(BATCH_ROWS, SEQ_LEN, NUM_KV_HEADS, group_size, HEAD_DIM), 2, 0)
        heads_out = lax.map(jax.checkpoint(head_group), (query_groups, jnp.moveaxis(key_rot, 2, 0), jnp.moveaxis(value_rows, 2, 0)))
        heads_flat = jnp.moveaxis(heads_out, 0, 2).reshape(BATCH_ROWS, SEQ_LEN, NUM_HEADS * HEAD_DIM)
        attn_sum = snap_bf16(jnp.dot(heads_flat, wo_f32))
        return snap_bf16(hidden_f32 + attn_sum)

    attn_out, pullback = jax.vjp(forward, hidden.astype(jnp.float32), norm_gain.astype(jnp.float32), w_query.astype(jnp.float32), w_key.astype(jnp.float32), w_value.astype(jnp.float32), w_out.astype(jnp.float32))
    grad_list = pullback(grad_out.astype(jnp.float32))
    return (attn_out.astype(jnp.bfloat16), grad_list[0].astype(jnp.bfloat16), grad_list[1], grad_list[2], grad_list[3], grad_list[4], grad_list[5])
```

```python
import functools

import jax
import jax.numpy as jnp
from jax import lax
from jax.experimental import pallas as pl
from jax.experimental.pallas import tpu as pltpu
from jax.sharding import PartitionSpec as P

HEAD_DIM = 128
NORM_EPS = 1e-5
ROPE_BASE = 10000.0
LOG2E = 1.4426950408889634
BF16 = jnp.bfloat16
F32 = jnp.float32
ANY = pl.BlockSpec(memory_space=pl.ANY)
VMEM_LIMIT = 62 * 1024 * 1024


def cost(flops, bytes_accessed):
    return pl.CostEstimate(flops=int(flops), bytes_accessed=int(bytes_accessed), transcendentals=0)


def params(n_axes=1):
    return pltpu.CompilerParams(dimension_semantics=("arbitrary",) * n_axes, vmem_limit_bytes=VMEM_LIMIT)


def norm_kernel(hidden_ref, gain_ref, out_ref):
    h = hidden_ref[0].astype(F32)
    inv = lax.rsqrt(jnp.mean(h * h, axis=-1, keepdims=True) + NORM_EPS)
    out_ref[...] = (h * inv * gain_ref[...].astype(F32)).astype(BF16)


def norm_row(hidden, gain2d, row):
    _, toks, width = hidden.shape
    blk = toks // 2
    return pl.pallas_call(
        norm_kernel,
        grid=(2,),
        out_shape=jax.ShapeDtypeStruct((toks, width), BF16),
        in_specs=[pl.BlockSpec((1, blk, width), lambda i: (row, i, 0)), pl.BlockSpec((1, width), lambda i: (0, 0))],
        out_specs=pl.BlockSpec((blk, width), lambda i: (i, 0)),
        compiler_params=params(),
        cost_estimate=cost(2e9, 4 * toks * width),
    )(hidden, gain2d)


def rotate(vals, cos_tab, sin_tab):
    lanes = vals.shape[-1]
    lane = lax.broadcasted_iota(jnp.int32, vals.shape, 1)
    swapped = jnp.where(lane % 2 == 0, pltpu.roll(vals, lanes - 1, 1), pltpu.roll(vals, 1, 1))
    return vals * cos_tab + swapped * sin_tab


def load_pieces(pieces, where_ref, lhs, sem):
    core = where_ref[1]
    copies = []
    for idx, piece in enumerate(pieces):
        rel_core, row = idx // 2, idx % 2
        slot = row * 2 + (core + rel_core) % 2
        copies.append(pltpu.make_async_copy(piece, lhs.at[slot], sem.at[idx]))
    for c in copies:
        c.start()
    for c in copies:
        c.wait()


def qkv_kernel(where_ref, p0, p1, p2, p3, wq, wk, wv, cos_ref, sin_ref, *rest):
    qo, ko, vo, lhs, sem = rest[-5:]
    step = pl.program_id(0)

    @pl.when(step == 0)
    def _():
        load_pieces((p0, p1, p2, p3), where_ref, lhs, sem)

    def emit(w_ref, o_ref, turn):
        for row in range(2):
            rows = lhs[2 * row:2 * row + 2].reshape(2 * lhs.shape[1], lhs.shape[2])
            val = jnp.dot(rows, w_ref[...], preferred_element_type=F32)
            if turn:
                c = cos_ref[row]
                s = sin_ref[row]
                val = rotate(val, jnp.concatenate([c, c], axis=1), jnp.concatenate([s, s], axis=1))
            o_ref[row] = val.astype(BF16)

    @pl.when(step < 2)
    def _():
        emit(wq, qo, True)

    @pl.when((step >= 2) & (step < 4))
    def _():
        emit(wk, ko, True)

    @pl.when(step >= 4)
    def _():
        emit(wv, vo, False)


def project_chunk(where, pieces, wq, wk, wv, cos_tab, sin_tab, bufs, seq):
    toks, width = pieces[0].shape
    cols = wq.shape[1]
    tile = cols // 2
    chunk = 2 * toks

    def wspec(first):
        return pl.BlockSpec((width, tile), lambda i, w: (0, jnp.clip(i - first, 0, 1)))

    def ospec(first):
        return pl.BlockSpec((2, chunk, tile), lambda i, w: (0, w[0], jnp.clip(i - first, 0, 1)))

    tab = pl.BlockSpec((2, chunk, HEAD_DIM), lambda i, w: (0, w[0], 0))
    extra = list(bufs) if bufs is not None else []
    n_in = 1 + 4 + 3 + 2
    return pl.pallas_call(
        qkv_kernel,
        grid_spec=pltpu.PrefetchScalarGridSpec(
            num_scalar_prefetch=1,
            grid=(6,),
            in_specs=[ANY] * 4 + [wspec(0), wspec(2), wspec(4), tab, tab] + [ANY] * len(extra),
            out_specs=[ospec(0), ospec(2), ospec(4)],
            scratch_shapes=[pltpu.VMEM((4, toks, width), BF16), pltpu.SemaphoreType.DMA((4,))],
        ),
        out_shape=[jax.ShapeDtypeStruct((2, seq, cols), BF16)] * 3,
        input_output_aliases={n_in + i: i for i in range(len(extra))},
        compiler_params=params(),
        cost_estimate=cost(2 * 2 * chunk * width * cols * 3, 16e6),
    )(where, *pieces, wq, wk, wv, cos_tab, sin_tab, *extra)


def heads_kernel(where_ref, p0, p1, p2, p3, w_ref, *rest):
    out_ref, lhs, sem = rest[-3:]

    @pl.when(pl.program_id(0) == 0)
    def _():
        load_pieces((p0, p1, p2, p3), where_ref, lhs, sem)

    for row in range(2):
        rows = lhs[2 * row:2 * row + 2].reshape(2 * lhs.shape[1], lhs.shape[2])
        out_ref[row] = lax.dot_general(rows, w_ref[...], (((1,), (1,)), ((), ())), preferred_element_type=F32).astype(BF16)


def grad_heads_chunk(where, pieces, w_out, buf, seq):
    toks, width = pieces[0].shape
    cols = w_out.shape[0]
    tile = cols // 2
    chunk = 2 * toks
    extra = [buf] if buf is not None else []
    return pl.pallas_call(
        heads_kernel,
        grid_spec=pltpu.PrefetchScalarGridSpec(
            num_scalar_prefetch=1,
            grid=(2,),
            in_specs=[ANY] * 4 + [pl.BlockSpec((tile, width), lambda i, w: (i, 0))] + [ANY] * len(extra),
            out_specs=pl.BlockSpec((2, chunk, tile), lambda i, w: (0, w[0], i)),
            scratch_shapes=[pltpu.VMEM((4, toks, width), BF16), pltpu.SemaphoreType.DMA((4,))],
        ),
        out_shape=jax.ShapeDtypeStruct((2, seq, cols), BF16),
        input_output_aliases={6: 0} if extra else {},
        compiler_params=params(),
        cost_estimate=cost(2 * 2 * chunk * width * cols, 9e6),
    )(where, *pieces, w_out, *extra)


def store_rel(out_ref, vals, block, where_ref, chips):
    half = vals.shape[0] // 2
    rel = lax.rem(block - where_ref[0] + chips, chips)
    for core in range(2):
        slot = rel * 2 + lax.rem(core + where_ref[1], 2)
        out_ref[0, pl.ds(pl.multiple_of(slot * half, half), half), :] = vals[core * half:(core + 1) * half]


def probs_t(k_ref, q_blk, pos_ref, block, size):
    n = (block + 1) * size
    s_t = lax.dot_general(k_ref[0, :n, :], q_blk, (((1,), (1,)), ((), ())), preferred_element_type=F32)
    key = lax.broadcasted_iota(jnp.int32, (n, size), 0)
    query = lax.broadcasted_iota(jnp.int32, (1, size), 1) + block * size
    first = query - pos_ref[0, :, block * size:n]
    s_t = jnp.where((key >= first) & (key <= query), s_t, -1e30)
    top = jnp.max(s_t, axis=0, keepdims=True)
    e = jnp.exp2((s_t - top) * (LOG2E * HEAD_DIM ** -0.5))
    return e * (1.0 / jnp.sum(e, axis=0, keepdims=True))


def attn_fwd_kernel(chips, where_ref, q_ref, k_ref, v_ref, pos_ref, o_ref):
    seq = q_ref.shape[1]
    size = seq // chips
    v_t = v_ref[0].T
    for block in range(chips):
        n = (block + 1) * size
        p_t = probs_t(k_ref, q_ref[0, block * size:n, :], pos_ref, block, size).astype(BF16)
        o_t = jnp.dot(v_t[:, :n], p_t, preferred_element_type=F32)
        store_rel(o_ref, o_t.T.astype(BF16), block, where_ref, chips)


def attn_bwd_kernel(chips, where_ref, q_ref, k_ref, v_ref, g_ref, pos_ref, cos_ref, sin_ref, dq_ref, dk_ref, dv_ref, dk_acc, dv_acc):
    seq = q_ref.shape[1]
    size = seq // chips
    k_t = k_ref[0].T
    for block in range(chips - 1, -1, -1):
        n = (block + 1) * size
        mine = slice(block * size, n)
        q_blk = q_ref[0, mine, :]
        g_blk = g_ref[0, mine, :]
        p_t = probs_t(k_ref, q_blk, pos_ref, block, size)
        dp_t = lax.dot_general(v_ref[0, :n, :], g_blk, (((1,), (1,)), ((), ())), preferred_element_type=F32)
        row_dot = jnp.sum(p_t * dp_t, axis=0, keepdims=True)
        ds_t = (p_t * (dp_t - row_dot) * (HEAD_DIM ** -0.5)).astype(BF16)
        dv_new = jnp.dot(p_t.astype(BF16), g_blk, preferred_element_type=F32)
        dk_new = jnp.dot(ds_t, q_blk, preferred_element_type=F32)
        if block == chips - 1:
            dv_acc[...] = dv_new
            dk_acc[...] = dk_new
        else:
            dv_acc[:n, :] += dv_new
            dk_acc[:n, :] += dk_new
        dq = jnp.dot(k_t[:, :n], ds_t, preferred_element_type=F32).T
        dq = rotate(dq, cos_ref[0, mine, :], -sin_ref[0, mine, :])
        store_rel(dq_ref, dq.astype(BF16), block, where_ref, chips)
    for block in range(chips):
        mine = slice(block * size, (block + 1) * size)
        dk = rotate(dk_acc[mine, :], cos_ref[0, mine, :], -sin_ref[0, mine, :])
        store_rel(dk_ref, dk.astype(BF16), block, where_ref, chips)
        store_rel(dv_ref, dv_acc[mine, :].astype(BF16), block, where_ref, chips)


def attention_specs(rows, seq, heads):
    head = pl.BlockSpec((1, seq, HEAD_DIM), lambda b, h, w: (b, 0, h))
    pos = pl.BlockSpec((1, 1, seq), lambda b, h, w: (b, 0, 0))
    tab = pl.BlockSpec((1, seq, HEAD_DIM), lambda b, h, w: (b, 0, 0))
    return head, pos, tab


def attention_fwd(chips, where, q, k, v, pos):
    rows, seq, cols = q.shape
    head, pos_spec, _ = attention_specs(rows, seq, cols // HEAD_DIM)
    return pl.pallas_call(
        functools.partial(attn_fwd_kernel, chips),
        grid_spec=pltpu.PrefetchScalarGridSpec(
            num_scalar_prefetch=1, grid=(rows, cols // HEAD_DIM),
            in_specs=[head, head, head, pos_spec], out_specs=head),
        out_shape=jax.ShapeDtypeStruct(q.shape, BF16),
        compiler_params=params(2),
        cost_estimate=cost(20e9, 8e6),
    )(where, q, k, v, pos)


def attention_bwd(chips, where, q, k, v, grad_o, pos, cos_tab, sin_tab):
    rows, seq, cols = q.shape
    head, pos_spec, tab = attention_specs(rows, seq, cols // HEAD_DIM)
    return pl.pallas_call(
        functools.partial(attn_bwd_kernel, chips),
        grid_spec=pltpu.PrefetchScalarGridSpec(
            num_scalar_prefetch=1, grid=(rows, cols // HEAD_DIM),
            in_specs=[head, head, head, head, pos_spec, tab, tab], out_specs=[head, head, head],
            scratch_shapes=[pltpu.VMEM((seq, HEAD_DIM), F32), pltpu.VMEM((seq, HEAD_DIM), F32)]),
        out_shape=[jax.ShapeDtypeStruct(q.shape, BF16)] * 3,
        compiler_params=params(2),
        cost_estimate=cost(40e9, 16e6),
    )(where, q, k, v, grad_o, pos, cos_tab, sin_tab)


def share_kernel(n_pairs, n_dest, transposed, *refs):
    lhs = refs[:n_pairs * n_dest]
    weights = refs[n_pairs * n_dest:n_pairs * n_dest + n_pairs]
    outs = refs[n_pairs * n_dest + n_pairs:]
    dims = (((1,), (1 if transposed else 0,)), ((), ()))
    for dest in range(n_dest):
        acc = None
        for pair in range(n_pairs):
            a = lhs[dest * n_pairs + pair][...]
            a = a.reshape(a.shape[0] * a.shape[1], a.shape[2])
            term = lax.dot_general(a, weights[pair][...], dims, preferred_element_type=F32)
            acc = term if acc is None else acc + term
        half = acc.shape[0] // 2
        for row in range(2):
            o = outs[dest * 2 + row]
            o[...] = acc[row * half:(row + 1) * half].astype(o.dtype)


def shares(toks, mine, partner, w_mine, w_partner, transposed, dests, dtypes):
    cols = mine[0].shape[2]
    width = w_mine[0].shape[0 if transposed else 1]
    tile = 512
    n_pairs = len(mine) + len(partner)
    in_specs, operands = [], []
    for d in dests:
        for a in mine:
            in_specs.append(pl.BlockSpec((2, toks, cols), lambda j, d=d: (0, 2 * d, 0)))
            operands.append(a)
        for a in partner:
            in_specs.append(pl.BlockSpec((2, toks, cols), lambda j, d=d: (0, d, 0)))
            operands.append(a)
    for w in list(w_mine) + list(w_partner):
        in_specs.append(pl.BlockSpec((tile, cols), lambda j: (j, 0)) if transposed else pl.BlockSpec((cols, tile), lambda j: (0, j)))
        operands.append(w)
    n_dest = len(dests)
    return pl.pallas_call(
        functools.partial(share_kernel, n_pairs, n_dest, transposed),
        grid=(width // tile,),
        out_shape=[jax.ShapeDtypeStruct((toks, width), dt) for dt in dtypes],
        in_specs=in_specs,
        out_specs=[pl.BlockSpec((toks, tile), lambda j: (0, j))] * (2 * n_dest),
        compiler_params=params(),
        cost_estimate=cost(2 * 2 * toks * n_dest * n_pairs * cols * width, n_pairs * cols * width * 2),
    )(*operands)


def solution(mesh):
    tp_size = mesh.shape['tp']
    chips = tp_size // 2

    def move(value, chip_step):
        return lax.ppermute(value, 'tp', [(2 * x + c, 2 * ((x + chip_step) % chips) + c) for x in range(chips) for c in range(2)])

    def swap(value):
        return lax.ppermute(value, 'tp', [(2 * x + c, 2 * x + 1 - c) for x in range(chips) for c in range(2)])

    def gather(r0, r1):
        left0, right1 = move(r0, 1), move(r1, -1)
        left1, right0 = move(r1, 1), move(r0, -1)
        far0, far1 = move(left0, 1), move(right1, -1)
        return {0: (r0, r1), 3: (left0, left1), 1: (right0, right1), 2: (far0, far1)}

    def reduce_scatter(make):
        two0, two1 = make((2,), (BF16, BF16))
        relay0, relay1 = move(two0, 1), move(two1, -1)
        one0, one1, three0, three1 = make((1, 3), (F32, BF16, BF16, F32))
        left1, right0 = move(one1, 1), move(three0, -1)
        one0 = (one0 + relay0.astype(F32)).astype(BF16)
        three1 = (three1 + relay1.astype(F32)).astype(BF16)
        left0, right1 = move(one0, 1), move(three1, -1)
        own0, own1 = make((0,), (F32, F32))
        return tuple(own + a.astype(F32) + b.astype(F32) for own, a, b in ((own0, left0, right0), (own1, left1, right1)))

    def device_step(hidden, positions, doc_ids, norm_gain, w_query, w_key, w_value, w_out, grad_out):
        rows, toks, width = hidden.shape
        seq = toks * tp_size
        me = lax.axis_index('tp')
        chip, core = me // 2, me % 2

        def where(step):
            return jnp.stack([(chip + step) % chips, core]).astype(jnp.int32)

        gain2d = norm_gain.reshape(1, width)
        normed = [norm_row(hidden, gain2d, row) for row in range(rows)]
        ring = gather(*normed)
        pos_full = lax.all_gather(positions, 'tp', axis=1, tiled=True)
        inv_freq = ROPE_BASE ** (-(2 * (jnp.arange(HEAD_DIM) // 2)).astype(F32) / HEAD_DIM)
        angles = pos_full.astype(F32)[:, :, None] * inv_freq
        cos_tab = jnp.cos(angles)
        sin_tab = jnp.where(jnp.arange(HEAD_DIM) % 2 == 0, -1.0, 1.0) * jnp.sin(angles)
        pos3 = pos_full.reshape(rows, 1, seq)
        other_w = [swap(w) for w in (w_out, w_query, w_key, w_value)]

        def with_partner(ring):
            return {s: (r[0], r[1], swap(r[0]), swap(r[1])) for s, r in ring.items()}

        pieces = with_partner(ring)
        bufs = None
        for step in (0, 1, 3, 2):
            bufs = project_chunk(where(step), pieces[step], w_query, w_key, w_value, cos_tab, sin_tab, bufs, seq)
        q, k, v = bufs
        here = where(0)
        heads_out = attention_fwd(chips, here, q, k, v, pos3)

        def for_partner(a):
            cols = a.shape[2]
            return swap(a.reshape(rows, chips, 2, toks, cols)[:, :, 1]).reshape(rows, chips * toks, cols)

        heads_other = for_partner(heads_out)
        sums = reduce_scatter(functools.partial(shares, toks, [heads_out], [heads_other], [w_out], [other_w[0]], False))
        attn_out = jnp.stack([hidden[r] + sums[r].astype(BF16) for r in range(rows)])

        grad_rows = [grad_out[r] for r in range(rows)]
        grad_pieces = with_partner(gather(*grad_rows))
        buf = None
        for step in (0, 1, 3, 2):
            buf = grad_heads_chunk(where(step), grad_pieces[step], w_out, buf, seq)
        dq, dk, dv = attention_bwd(chips, here, q, k, v, buf, pos3, cos_tab, sin_tab)
        grads = [dq, dk, dv]
        others = [for_partner(a) for a in grads]
        grad_normed = jnp.stack(reduce_scatter(functools.partial(
            shares, toks, grads, others, [w_query, w_key, w_value], other_w[1:], True)))

        def whole(pieces):
            return jnp.concatenate([pieces[s][2 * c + r] for r in range(rows) for s in range(chips) for c in range(2)], axis=0)

        def weight_grad(a, b):
            return lax.dot_general(a, b, (((0,), (0,)), ((), ())), preferred_element_type=F32)

        grad_w_out = weight_grad(heads_out.reshape(rows * seq, -1), whole(grad_pieces))
        normed_all = whole(pieces)
        grad_wq, grad_wk, grad_wv = (weight_grad(normed_all, a.reshape(rows * seq, -1)) for a in grads)

        hidden_f = hidden.astype(F32)
        inv_rms = lax.rsqrt(jnp.mean(hidden_f * hidden_f, axis=-1, keepdims=True) + NORM_EPS)
        scaled = grad_normed * norm_gain.astype(F32)
        grad_gain = jnp.sum(grad_normed * hidden_f * inv_rms, axis=(0, 1))
        mean_term = jnp.mean(scaled * hidden_f, axis=-1, keepdims=True)
        grad_norm_in = inv_rms * scaled - hidden_f * (inv_rms * inv_rms * inv_rms) * mean_term
        grad_hidden = (grad_out.astype(F32) + grad_norm_in).astype(BF16)
        grad_gain = grad_gain + swap(grad_gain)
        for turn in (0, 1):
            pairs = [(x, x ^ 1) if turn == 0 else (x, chips - 1 - x) for x in range(chips)]
            grad_gain = grad_gain + lax.ppermute(grad_gain, 'tp', [(2 * a + c, 2 * b + c) for a, b in pairs for c in range(2)])
        return (attn_out, grad_hidden, grad_gain, grad_wq, grad_wk, grad_wv, grad_w_out)

    row_spec = P('dp', 'tp', None)
    tok_spec = P('dp', 'tp')
    col_spec = P(None, 'tp')
    return jax.shard_map(
        device_step, mesh=mesh,
        in_specs=(row_spec, tok_spec, tok_spec, P(), col_spec, col_spec, col_spec, P('tp', None), row_spec),
        out_specs=(row_spec, row_spec, P('dp'), P('dp', 'tp'), P('dp', 'tp'), P('dp', 'tp'), P(('dp', 'tp'), None)),
        check_vma=False)
```

```python
import functools

import jax
import jax.numpy as jnp
from jax import lax
from jax.experimental import pallas as pl
from jax.experimental.pallas import tpu as pltpu
from jax.sharding import PartitionSpec as P


HEAD_DIM = 128
NORM_EPS = 1e-5
ROPE_BASE = 10000.0
LOG2E = 1.4426950408889634
BF16 = jnp.bfloat16
F32 = jnp.float32
ANY = pl.BlockSpec(memory_space=pl.ANY)
VMEM_LIMIT = 62 * 1024 * 1024


def cost(flops, bytes_accessed):
    return pl.CostEstimate(flops=int(flops), bytes_accessed=int(bytes_accessed), transcendentals=0)


def params(n_axes=1):
    return pltpu.CompilerParams(dimension_semantics=("arbitrary",) * n_axes, vmem_limit_bytes=VMEM_LIMIT)


def norm_kernel(hidden_ref, gain_ref, out_ref):
    h = hidden_ref[0].astype(F32)
    inv = lax.rsqrt(jnp.mean(h * h, axis=-1, keepdims=True) + NORM_EPS)
    out_ref[...] = (h * inv * gain_ref[...].astype(F32)).astype(BF16)


def norm_row(hidden, gain2d, row):
    _, toks, width = hidden.shape
    blk = toks // 2
    return pl.pallas_call(
        norm_kernel,
        grid=(2,),
        out_shape=jax.ShapeDtypeStruct((toks, width), BF16),
        in_specs=[pl.BlockSpec((1, blk, width), lambda i: (row, i, 0)), pl.BlockSpec((1, width), lambda i: (0, 0))],
        out_specs=pl.BlockSpec((blk, width), lambda i: (i, 0)),
        compiler_params=params(),
        cost_estimate=cost(2e9, 4 * toks * width),
    )(hidden, gain2d)


def rotate(vals, cos_tab, sin_tab):
    lanes = vals.shape[-1]
    lane = lax.broadcasted_iota(jnp.int32, vals.shape, 1)
    swapped = jnp.where(lane % 2 == 0, pltpu.roll(vals, lanes - 1, 1), pltpu.roll(vals, 1, 1))
    return vals * cos_tab + swapped * sin_tab


K_PARTS = 4


def split_pieces(pieces):
    return [p if not isinstance(p, tuple) else p[0] for p in pieces], tuple(None if not isinstance(p, tuple) else p[1] for p in pieces)


def row_refs(refs, picks):
    return [r if pick is None else r.at[pick] for r, pick in zip(refs, picks)]


def here(chips):
    me = lax.axis_index('tp')
    return lax.rem(me // 2, chips), lax.rem(me, 2)


def project_kernel(chips, steps, picks, turns, flipped, own_tabs, has_tabs, *refs):
    n, n_w = len(steps), len(turns)
    chip, core = here(chips)
    blocks = [lax.rem(chip + step, chips) for step in steps]
    pieces = row_refs(refs[:4 * n], picks)
    weights = refs[4 * n:4 * n + n_w]
    tabs = refs[4 * n + n_w:4 * n + n_w + 2] if has_tabs else ()
    lhs, wbuf, acc, tab, stage, lhs_sem, w_sem, tab_sem, out_sem = refs[-9:]
    outs = refs[-9 - n_w:-9]
    toks = pieces[0].shape[0]
    part = lhs.shape[2]
    cols = outs[0].shape[2]
    chunk = 2 * toks

    def fetch(k):
        at = pl.ds(pl.multiple_of(k * part, part), part)
        for w in range(n_w):
            if flipped:
                yield pltpu.make_async_copy(weights[w].at[:, at], wbuf.at[k, pl.ds(w * cols, cols), :], w_sem.at[k, w])
            else:
                yield pltpu.make_async_copy(weights[w].at[at, :], wbuf.at[k, :, pl.ds(w * cols, cols)], w_sem.at[k, w])
        for idx, piece in enumerate(pieces):
            c, rel_core, row = idx // 4, (idx % 4) // 2, idx % 2
            slot = 4 * c + 2 * row + lax.rem(core + rel_core, 2)
            yield pltpu.make_async_copy(
                piece.at[:, at], lhs.at[k, pl.ds(pl.multiple_of(slot * toks, toks), toks), :], lhs_sem.at[k, idx])

    def fetch_tabs():
        for c in range(n):
            first = 0 if own_tabs else pl.multiple_of(blocks[c] * chunk, chunk)
            for t, ref in enumerate(tabs):
                yield pltpu.make_async_copy(ref.at[:, pl.ds(first, chunk), :], tab.at[c, t], tab_sem.at[c, t])

    for k in range(K_PARTS):
        for copy in fetch(k):
            copy.start()
    for copy in fetch_tabs():
        copy.start()
    acc[...] = jnp.zeros_like(acc)

    def body(k, carry):
        for copy in fetch(k):
            copy.wait()

        def one(c, carry):
            at = pl.ds(pl.multiple_of(c * 4 * toks, 4 * toks), 4 * toks)
            acc[at, :] += lax.dot_general(lhs[k, at, :], wbuf[k], (((1,), (1 if flipped else 0,)), ((), ())), preferred_element_type=F32)
            return carry

        return lax.fori_loop(0, n, one, carry) if n > 1 else one(0, carry)

    lax.fori_loop(0, K_PARTS, body, 0)
    for copy in fetch_tabs():
        copy.wait()

    def give(w, c):
        at = pl.ds(pl.multiple_of(blocks[c] * chunk, chunk), chunk)
        return pltpu.make_async_copy(stage.at[w, c], outs[w].at[:, at, :], out_sem.at[w, c])

    for w, turn in enumerate(turns):
        def finish(idx, carry, w=w, turn=turn):
            c, row = idx // 2, lax.rem(idx, 2)
            at = pl.ds(pl.multiple_of(idx * chunk, chunk), chunk)
            for head in range(cols // HEAD_DIM):
                lanes = slice(head * HEAD_DIM, (head + 1) * HEAD_DIM)
                val = acc[at, w * cols + head * HEAD_DIM:w * cols + (head + 1) * HEAD_DIM]
                if turn:
                    val = rotate(val, tab[c, 0, row], tab[c, 1, row])
                stage[w, c, row, :, lanes] = val.astype(BF16)
            return carry

        lax.fori_loop(0, 2 * n, finish, 0)
        for c in range(n):
            give(w, c).start()
    for w in range(n_w):
        for c in range(n):
            give(w, c).wait()


def project(chips, steps, chunks, weights, turns, tabs, bufs, seq, flipped=False, own_tabs=False):
    pieces, picks = split_pieces([p for c in chunks for p in c])
    toks, width = pieces[0].shape[-2:]
    cols = weights[0].shape[0 if flipped else 1]
    n, n_w = len(chunks), len(weights)
    part = width // K_PARTS
    extra = list(bufs) if bufs is not None else []
    n_in = len(pieces) + n_w + len(tabs)
    w_shape = (K_PARTS, n_w * cols, part) if flipped else (K_PARTS, part, n_w * cols)
    return pl.pallas_call(
        functools.partial(project_kernel, chips, steps, picks, turns, flipped, own_tabs, bool(tabs)),
        grid_spec=pltpu.PrefetchScalarGridSpec(
            num_scalar_prefetch=0,
            grid=(1,),
            in_specs=[ANY] * (n_in + len(extra)),
            out_specs=[ANY] * n_w,
            scratch_shapes=[
                pltpu.VMEM((K_PARTS, 4 * n * toks, part), BF16), pltpu.VMEM(w_shape, BF16),
                pltpu.VMEM((4 * n * toks, n_w * cols), F32), pltpu.VMEM((n, 2, 2, 2 * toks, HEAD_DIM), F32),
                pltpu.VMEM((n_w, n, 2, 2 * toks, cols), BF16),
                pltpu.SemaphoreType.DMA((K_PARTS, 4 * n)), pltpu.SemaphoreType.DMA((K_PARTS, n_w)),
                pltpu.SemaphoreType.DMA((n, 2)), pltpu.SemaphoreType.DMA((n_w, n))],
        ),
        out_shape=[jax.ShapeDtypeStruct((2, seq, cols), BF16)] * n_w,
        input_output_aliases={n_in + i: i for i in range(len(extra))},
        compiler_params=params(),
        cost_estimate=cost(2 * 4 * toks * n * width * cols * n_w, 16e6),
    )(*pieces, *weights, *tabs, *extra)


def weight_grad_kernel(n_pieces, picks, n_acts, acts_left, first, *refs):
    pieces, acts = row_refs(refs[:n_pieces], picks), refs[n_pieces:n_pieces + n_acts]
    if acts_left:
        *refs, act_t = refs
    act, tiles, piece_sem, act_sem = refs[-4:]
    n_out = 1 if acts_left else n_acts // 2
    outs = refs[-4 - n_out:-4]
    step, steps = pl.program_id(0), pl.num_programs(0)
    toks = pieces[0].shape[0]
    cols = acts[0].shape[2]
    seq = 2 * acts[0].shape[1]
    tile = tiles.shape[2]

    def fetch(at, slot):
        for idx, piece in enumerate(pieces):
            yield pltpu.make_async_copy(
                piece.at[:, pl.ds(pl.multiple_of((at + first) * tile, tile), tile)],
                tiles.at[slot, pl.ds(idx * toks, toks), :], piece_sem.at[slot, idx])

    def fetch_acts():
        for idx, a in enumerate(acts):
            for row in range(2):
                yield pltpu.make_async_copy(
                    a.at[row], act.at[pl.ds((2 * row + idx % 2) * seq // 2, seq // 2), pl.ds(idx // 2 * cols, cols)],
                    act_sem.at[2 * idx + row])

    slot = lax.rem(step, 2)

    @pl.when(step == 0)
    def _():
        for c in fetch_acts():
            c.start()
        for c in fetch(0, 0):
            c.start()
        for c in fetch_acts():
            c.wait()
        if acts_left:
            act_t[...] = act[...].T

    @pl.when(step + 1 < steps)
    def _():
        for c in fetch(step + 1, 1 - slot):
            c.start()

    for c in fetch(step, slot):
        c.wait()
    dims = (((0,), (0,)), ((), ()))
    if acts_left:
        outs[0][...] = jnp.dot(act_t[...], tiles[slot], preferred_element_type=F32)
    else:
        res = lax.dot_general(tiles[slot], act[...], dims, preferred_element_type=F32)
        for idx, o in enumerate(outs):
            o[...] = res[:, idx * cols:(idx + 1) * cols]


def weight_grad(pieces, acts, acts_left, half=None, bufs=()):
    pieces, picks = split_pieces(pieces)
    _, width = pieces[0].shape[-2:]
    seq, cols = 2 * acts[0].shape[1], acts[0].shape[2]
    tile = 512
    n_acts = len(acts) // 2
    steps = width // tile if half is None else width // tile // 2
    first = (half or 0) * steps
    if acts_left:
        out_shape = [jax.ShapeDtypeStruct((cols, width), F32)]
        out_specs = [pl.BlockSpec((cols, tile), lambda i: (0, first + i))]
    else:
        out_shape = [jax.ShapeDtypeStruct((width, cols), F32)] * n_acts
        out_specs = [pl.BlockSpec((tile, cols), lambda i: (first + i, 0))] * n_acts
    n_in = len(pieces) + len(acts)
    return pl.pallas_call(
        functools.partial(weight_grad_kernel, len(pieces), picks, len(acts), acts_left, first),
        grid=(steps,),
        in_specs=[ANY] * (n_in + len(bufs)),
        out_specs=out_specs,
        out_shape=out_shape,
        scratch_shapes=[pltpu.VMEM((2 * seq, n_acts * cols), BF16), pltpu.VMEM((2, 2 * seq, tile), BF16),
                        pltpu.SemaphoreType.DMA((2, len(pieces))), pltpu.SemaphoreType.DMA((4 * n_acts,))]
                       + ([pltpu.VMEM((cols, 2 * seq), BF16)] if acts_left else []),
        input_output_aliases={n_in + i: i for i in range(len(bufs))},
        compiler_params=params(),
        cost_estimate=cost(2 * 2 * seq * steps * tile * cols * n_acts, 40e6),
    )(*pieces, *acts, *bufs)


def store_rel(halves, vals, block, chips):
    half = vals.shape[0] // 2
    chip, mine = here(chips)
    rel = lax.rem(block - chip + chips, chips)
    for core in range(2):
        halves[lax.rem(core + mine, 2), pl.ds(pl.multiple_of(rel * half, half), half), :] = vals[core * half:(core + 1) * half]


def probs_t(k_ref, q_blk, pos_ref, block, size):
    n = (block + 1) * size
    s_t = lax.dot_general(k_ref[0, :n, :], q_blk, (((1,), (1,)), ((), ())), preferred_element_type=F32)
    key = lax.broadcasted_iota(jnp.int32, (n, size), 0)
    query = lax.broadcasted_iota(jnp.int32, (1, size), 1) + block * size
    first = query - pos_ref[0, :, block * size:n]
    old = n - size
    near = jnp.where((key[old:] >= first) & (key[old:] <= query), s_t[old:], -1e30)
    s_t = jnp.concatenate([jnp.where(key[:old] >= first, s_t[:old], -1e30), near], axis=0) if old else near
    top = jnp.max(s_t, axis=0, keepdims=True)
    e = jnp.exp2((s_t - top) * (LOG2E * HEAD_DIM ** -0.5))
    return e * (1.0 / jnp.sum(e, axis=0, keepdims=True))


def attn_fwd_kernel(chips, q_ref, k_ref, v_ref, pos_ref, o_mine, o_theirs, o_halves):
    seq = q_ref.shape[1]
    size = seq // chips
    v_t = v_ref[0].T
    for block in range(chips):
        n = (block + 1) * size
        p_t = probs_t(k_ref, q_ref[0, block * size:n, :], pos_ref, block, size).astype(BF16)
        o_t = jnp.dot(v_t[:, :n], p_t, preferred_element_type=F32)
        store_rel(o_halves, o_t.T.astype(BF16), block, chips)
    o_mine[0] = o_halves[0]
    o_theirs[0] = o_halves[1]


def attn_bwd_kernel(chips, q_ref, k_ref, v_ref, g_ref, pos_ref, cos_ref, sin_ref, *refs):
    outs, (dk_acc, dv_acc, dq_halves, dk_halves, dv_halves) = refs[:6], refs[6:]
    seq = q_ref.shape[1]
    size = seq // chips
    k_t = k_ref[0].T
    for block in range(chips - 1, -1, -1):
        n = (block + 1) * size
        mine = slice(block * size, n)
        q_blk = q_ref[0, mine, :]
        g_blk = g_ref[0, mine, :]
        p_t = probs_t(k_ref, q_blk, pos_ref, block, size)
        dp_t = lax.dot_general(v_ref[0, :n, :], g_blk, (((1,), (1,)), ((), ())), preferred_element_type=F32)
        row_dot = jnp.sum(p_t * dp_t, axis=0, keepdims=True)
        ds_t = (p_t * (dp_t - row_dot) * (HEAD_DIM ** -0.5)).astype(BF16)
        dv_new = jnp.dot(p_t.astype(BF16), g_blk, preferred_element_type=F32)
        dk_new = jnp.dot(ds_t, q_blk, preferred_element_type=F32)
        if block == chips - 1:
            dv_acc[...] = dv_new
            dk_acc[...] = dk_new
        else:
            dv_acc[:n, :] += dv_new
            dk_acc[:n, :] += dk_new
        dq = jnp.dot(k_t[:, :n], ds_t, preferred_element_type=F32).T
        dq = rotate(dq, cos_ref[0, mine, :], -sin_ref[0, mine, :])
        store_rel(dq_halves, dq.astype(BF16), block, chips)
    for block in range(chips):
        mine = slice(block * size, (block + 1) * size)
        dk = rotate(dk_acc[mine, :], cos_ref[0, mine, :], -sin_ref[0, mine, :])
        store_rel(dk_halves, dk.astype(BF16), block, chips)
        store_rel(dv_halves, dv_acc[mine, :].astype(BF16), block, chips)
    for idx, halves in enumerate((dq_halves, dk_halves, dv_halves)):
        outs[2 * idx][0] = halves[0]
        outs[2 * idx + 1][0] = halves[1]


def attention_specs(seq):
    head = pl.BlockSpec((1, seq, HEAD_DIM), lambda b, h: (b, 0, h))
    half = pl.BlockSpec((1, seq // 2, HEAD_DIM), lambda b, h: (b, 0, h))
    pos = pl.BlockSpec((1, 1, seq), lambda b, h: (b, 0, 0))
    tab = pl.BlockSpec((1, seq, HEAD_DIM), lambda b, h: (b, 0, 0))
    return head, half, pos, tab


def attention_fwd(chips, q, k, v, pos):
    rows, seq, cols = q.shape
    head, half, pos_spec, _ = attention_specs(seq)
    return pl.pallas_call(
        functools.partial(attn_fwd_kernel, chips),
        grid=(rows, cols // HEAD_DIM),
        in_specs=[head, head, head, pos_spec], out_specs=[half] * 2,
        scratch_shapes=[pltpu.VMEM((2, seq // 2, HEAD_DIM), BF16)],
        out_shape=[jax.ShapeDtypeStruct((rows, seq // 2, cols), BF16)] * 2,
        compiler_params=params(2),
        cost_estimate=cost(20e9, 8e6),
    )(q, k, v, pos)


def attention_bwd(chips, q, k, v, grad_o, pos, cos_tab, sin_tab):
    rows, seq, cols = q.shape
    head, half, pos_spec, tab = attention_specs(seq)
    return pl.pallas_call(
        functools.partial(attn_bwd_kernel, chips),
        grid=(rows, cols // HEAD_DIM),
        in_specs=[head, head, head, head, pos_spec, tab, tab], out_specs=[half] * 6,
        scratch_shapes=[pltpu.VMEM((seq, HEAD_DIM), F32)] * 2 + [pltpu.VMEM((2, seq // 2, HEAD_DIM), BF16)] * 3,
        out_shape=[jax.ShapeDtypeStruct((rows, seq // 2, cols), BF16)] * 6,
        compiler_params=params(2),
        cost_estimate=cost(40e9, 16e6),
    )(q, k, v, grad_o, pos, cos_tab, sin_tab)


def share_kernel(n_pairs, n_dest, flipped, *refs):
    lhs = refs[:n_pairs * n_dest]
    weights = refs[n_pairs * n_dest:n_pairs * n_dest + n_pairs]
    outs = refs[-2 * n_dest:]
    acc = None
    for pair in range(n_pairs):
        parts = [lhs[dest * n_pairs + pair][...] for dest in range(n_dest)]
        a = jnp.concatenate([p.reshape(p.shape[0] * p.shape[1], p.shape[2]) for p in parts], axis=0)
        term = lax.dot_general(a, weights[pair][...], (((1,), (1 if flipped else 0,)), ((), ())), preferred_element_type=F32)
        acc = term if acc is None else acc + term
    half = acc.shape[0] // (2 * n_dest)
    for idx, o in enumerate(outs):
        o[...] = acc[idx * half:(idx + 1) * half].astype(o.dtype)


def shares(toks, mine, partner, weights, flipped, dests, dtypes, deps=()):
    cols = mine[0].shape[2]
    width = weights[0].shape[0 if flipped else 1]
    tile = 512 if len(dests) > 1 and flipped else 1024
    n_pairs = len(mine) + len(partner)
    in_specs, operands = [], []
    for d in dests:
        for a in list(mine) + list(partner):
            in_specs.append(pl.BlockSpec((2, toks, cols), lambda j, d=d: (0, d, 0)))
            operands.append(a)
    w_spec = pl.BlockSpec((tile, cols), lambda j: (j, 0)) if flipped else pl.BlockSpec((cols, tile), lambda j: (0, j))
    in_specs += [w_spec] * len(weights) + [ANY] * len(deps)
    n_dest = len(dests)
    return pl.pallas_call(
        functools.partial(share_kernel, n_pairs, n_dest, flipped),
        grid=(width // tile,),
        out_shape=[jax.ShapeDtypeStruct((toks, width), dt) for dt in dtypes],
        in_specs=in_specs,
        out_specs=[pl.BlockSpec((toks, tile), lambda j: (0, j))] * (2 * n_dest),
        compiler_params=params(),
        cost_estimate=cost(2 * 2 * toks * n_dest * n_pairs * cols * width, n_pairs * cols * width * 2),
    )(*operands, *weights, *deps)


SUB_ROWS = 16


def by_rows(block, fn):
    def body(i, carry):
        fn(pl.ds(pl.multiple_of(i * SUB_ROWS, SUB_ROWS), SUB_ROWS))
        return carry

    lax.fori_loop(0, block // SUB_ROWS, body, 0)


def tail_kernel(h_ref, g_ref, gain_ref, own0, own1, left0, left1, right0, right1, out_ref, gg_ref, gg_acc):
    step = pl.program_id(0)

    @pl.when(step == 0)
    def _():
        gg_acc[...] = jnp.zeros_like(gg_acc)

    def finish(own, left, right):
        def some(at):
            h = h_ref[0, at, :].astype(F32)
            inv = lax.rsqrt(jnp.mean(h * h, axis=-1, keepdims=True) + NORM_EPS)
            grad = own[at, :] + left[at, :].astype(F32) + right[at, :].astype(F32)
            unit = grad * (h * inv)
            gg_acc[...] += unit[:8] + unit[8:]
            scaled = grad * gain_ref[...].astype(F32)
            mean_term = jnp.mean(scaled * h, axis=-1, keepdims=True)
            out_ref[0, at, :] = (g_ref[0, at, :].astype(F32) + inv * scaled - h * (inv * inv * inv) * mean_term).astype(BF16)

        by_rows(h_ref.shape[1], some)

    @pl.when(step < 2)
    def _():
        finish(own0, left0, right0)

    @pl.when(step >= 2)
    def _():
        finish(own1, left1, right1)

    @pl.when(step == 3)
    def _():
        gg_ref[...] = jnp.sum(gg_acc[...], axis=0, keepdims=True)


def row_specs(toks, width):
    blk = toks // 2
    whole = pl.BlockSpec((1, blk, width), lambda i: (i // 2, i % 2, 0))
    return whole, [pl.BlockSpec((blk, width), lambda i, r=r: (jnp.clip(i - 2 * r, 0, 1), 0)) for r in range(2)]


def finish_norm(hidden, grad_out, gain2d, own, left, right):
    _, toks, width = hidden.shape
    whole, per_row = row_specs(toks, width)
    one = pl.BlockSpec((1, width), lambda i: (0, 0))
    return pl.pallas_call(
        tail_kernel,
        grid=(4,),
        out_shape=[jax.ShapeDtypeStruct(hidden.shape, BF16), jax.ShapeDtypeStruct((1, width), F32)],
        in_specs=[whole, whole, one] + per_row * 3,
        out_specs=[whole, one],
        scratch_shapes=[pltpu.VMEM((8, width), F32)],
        compiler_params=params(),
        cost_estimate=cost(4e9, 14e6),
    )(hidden, grad_out, gain2d, *own, *left, *right)


def residual_kernel(h_ref, own0, own1, left0, left1, right0, right1, out_ref):
    step = pl.program_id(0)

    def finish(own, left, right):
        def some(at):
            attn = (own[at, :] + left[at, :].astype(F32) + right[at, :].astype(F32)).astype(BF16)
            out_ref[0, at, :] = (h_ref[0, at, :].astype(F32) + attn.astype(F32)).astype(BF16)

        by_rows(h_ref.shape[1], some)

    @pl.when(step < 2)
    def _():
        finish(own0, left0, right0)

    @pl.when(step >= 2)
    def _():
        finish(own1, left1, right1)


def finish_residual(hidden, own, left, right):
    _, toks, width = hidden.shape
    whole, per_row = row_specs(toks, width)
    return pl.pallas_call(
        residual_kernel,
        grid=(4,),
        out_shape=jax.ShapeDtypeStruct(hidden.shape, BF16),
        in_specs=[whole] + per_row * 3,
        out_specs=whole,
        compiler_params=params(),
        cost_estimate=cost(1e9, 12e6),
    )(hidden, *own, *left, *right)


def relay_kernel(a0, a1, b0, b1, o0, o1):
    def some(at):
        o0[at, :] = (a0[at, :] + b0[at, :].astype(F32)).astype(BF16)
        o1[at, :] = (a1[at, :] + b1[at, :].astype(F32)).astype(BF16)

    by_rows(a0.shape[0], some)


def relay(own, received):
    toks, width = own[0].shape
    spec = pl.BlockSpec((toks // 4, width), lambda i: (i, 0))
    return pl.pallas_call(
        relay_kernel,
        grid=(4,),
        out_shape=[jax.ShapeDtypeStruct((toks, width), BF16)] * 2,
        in_specs=[spec] * 4,
        out_specs=[spec] * 2,
        compiler_params=params(),
        cost_estimate=cost(1e9, 8e6),
    )(*own, *received)


def solution(mesh):
    tp_size = mesh.shape['tp']
    chips = tp_size // 2

    def move(value, chip_step):
        return lax.ppermute(value, 'tp', [(2 * x + c, 2 * ((x + chip_step) % chips) + c) for x in range(chips) for c in range(2)])

    def swap(value):
        return lax.ppermute(value, 'tp', [(2 * x + c, 2 * x + 1 - c) for x in range(chips) for c in range(2)])

    def device_step(hidden, positions, doc_ids, norm_gain, w_query, w_key, w_value, w_out, grad_out):
        rows, toks, width = hidden.shape
        seq = toks * tp_size
        me = lax.axis_index('tp')
        chip, core = me // 2, me % 2

        def both_cores(own, other):
            return jnp.where(core == 0, jnp.concatenate([own, other], axis=-1), jnp.concatenate([other, own], axis=-1))

        def tables(pos):
            inv_freq = ROPE_BASE ** (-(2 * (jnp.arange(HEAD_DIM) // 2)).astype(F32) / HEAD_DIM)
            angles = pos.astype(F32)[:, :, None] * inv_freq
            return jnp.cos(angles), jnp.where(jnp.arange(HEAD_DIM) % 2 == 0, -1.0, 1.0) * jnp.sin(angles)

        in_w, turns = [w_query, w_key, w_value], (True, True, False)

        gain2d = norm_gain.reshape(1, width)
        own_pos = both_cores(positions, swap(positions))

        def both_rows(a):
            return (a, 0), (a, 1)

        g0, g1 = grad_out[0], grad_out[1]
        grad_pieces = {0: (*both_rows(grad_out), *both_rows(swap(grad_out)))}
        buf = project(chips, (0,), [grad_pieces[0]], [w_out], (False,), (), None, seq, flipped=True)
        n0 = norm_row(hidden, gain2d, 0)
        n1 = norm_row(hidden, gain2d, 1)
        left0, right1 = move(n0, 1), move(n1, -1)
        pieces = {0: (n0, n1, swap(n0), swap(n1))}
        far_pos = [move(own_pos, -1), move(own_pos, 2), move(own_pos, 1)]
        left1, right0 = move(n1, 1), move(n0, -1)
        other_w = [swap(w) for w in (w_out, w_query, w_key, w_value)]
        qkv = project(chips, (0,), [pieces[0]], in_w, turns, tables(own_pos), None, seq, own_tabs=True)
        *far_pos, q0 = lax.optimization_barrier((*far_pos, qkv[0]))
        qkv = [q0, *qkv[1:]]
        pos_rel = jnp.stack([own_pos, *far_pos], axis=1)
        far0, far1 = move(left0, 1), move(right1, -1)

        g_left0, g_right1 = move(g0, 1), move(g1, -1)
        g_left1, g_right0 = move(g1, 1), move(g0, -1)

        twice = jnp.concatenate([pos_rel, pos_rel], axis=1)
        pos_full = lax.dynamic_slice_in_dim(twice, (chips - chip) % chips, chips, axis=1).reshape(rows, seq)
        pos3 = pos_full.reshape(rows, 1, seq)
        tabs = cos_tab, sin_tab = tables(pos_full)
        pieces[3] = (left0, left1, swap(left0), swap(left1))
        pieces[1] = (right0, right1, swap(right0), swap(right1))
        qkv = project(chips, (1, 3), [pieces[1], pieces[3]], in_w, turns, tabs, qkv, seq)
        pieces[2] = (far0, far1, swap(far0), swap(far1))
        q, k, v = project(chips, (2,), [pieces[2]], in_w, turns, tabs, qkv, seq)
        w_out_both = [w_out, other_w[0]]
        in_both = in_w + other_w[1:]
        g_far0, g_far1 = move(g_left0, 1), move(g_right1, -1)
        grad_pieces[3] = (g_left0, g_left1, swap(g_left0), swap(g_left1))
        grad_pieces[1] = (g_right0, g_right1, swap(g_right0), swap(g_right1))
        grad_pieces[2] = (g_far0, g_far1, swap(g_far0), swap(g_far1))
        o_mine, o_theirs = attention_fwd(chips, q, k, v, pos3)

        share_o = functools.partial(shares, toks, [o_mine], [swap(o_theirs)], w_out_both, False)
        o_two0, o_two1, o_one0, o_one1, o_three0, o_three1, *o_own = share_o(
            (2, 1, 3, 0), (BF16, BF16, F32, BF16, BF16, F32, F32, F32))
        o_relay = move(o_two0, 1), move(o_two1, -1)
        o_left1, o_right0 = move(o_one1, 1), move(o_three0, -1)

        buf = project(chips, (1, 3), [grad_pieces[s] for s in (1, 3)], [w_out], (False,), (), buf, seq, flipped=True)
        (buf,) = project(chips, (2,), [grad_pieces[2]], [w_out], (False,), (), buf, seq, flipped=True)
        o_one0, o_three1 = relay((o_one0, o_three1), o_relay)
        o_left0, o_right1 = move(o_one0, 1), move(o_three1, -1)
        grads = attention_bwd(chips, q, k, v, buf, pos3, cos_tab, sin_tab)

        def whole(pieces):
            return [pieces[s][2 * c + r] for r in range(rows) for c in range(2) for s in range(chips)]

        grad_w_out = weight_grad(whole(grad_pieces), [o_mine, o_theirs], True, 0)
        share_g = functools.partial(shares, toks, grads[::2], [swap(a) for a in grads[1::2]], in_both, True)
        g_two = share_g((2,), (BF16, BF16))
        g_relay = move(g_two[0], 1), move(g_two[1], -1)
        g_one0, g_one1, g_three0, g_three1, g_own0, g_own1 = share_g((1, 3, 0), (F32, BF16, BF16, F32, F32, F32))
        d_left1, d_right0 = move(g_one1, 1), move(g_three0, -1)

        (grad_w_out,) = weight_grad(whole(grad_pieces), [o_mine, o_theirs], True, 1, grad_w_out)
        g_one0, g_three1 = relay((g_one0, g_three1), g_relay)
        d_left0, d_right1 = move(g_one0, 1), move(g_three1, -1)
        grad_wq, grad_wk, grad_wv = weight_grad(whole(pieces), grads, False)
        attn_out = finish_residual(hidden, o_own, (o_left0, o_left1), (o_right0, o_right1))

        grad_hidden, grad_gain = finish_norm(hidden, grad_out, gain2d, (g_own0, g_own1), (d_left0, d_left1), (d_right0, d_right1))
        grad_gain = grad_gain.reshape(width)
        grad_gain = grad_gain + swap(grad_gain)
        for turn in (0, 1):
            pairs = [(x, x ^ 1) if turn == 0 else (x, chips - 1 - x) for x in range(chips)]
            grad_gain = grad_gain + lax.ppermute(grad_gain, 'tp', [(2 * a + c, 2 * b + c) for a, b in pairs for c in range(2)])
        return (attn_out, grad_hidden, grad_gain, grad_wq, grad_wk, grad_wv, grad_w_out)

    row_spec = P('dp', 'tp', None)
    tok_spec = P('dp', 'tp')
    col_spec = P(None, 'tp')
    return jax.shard_map(
        device_step, mesh=mesh,
        in_specs=(row_spec, tok_spec, tok_spec, P(), col_spec, col_spec, col_spec, P('tp', None), row_spec),
        out_specs=(row_spec, row_spec, P('dp'), P('dp', 'tp'), P('dp', 'tp'), P('dp', 'tp'), P(('dp', 'tp'), None)),
        check_vma=False)
```

```python
import functools

import jax
import jax.numpy as jnp
from jax import lax
from jax.experimental import pallas as pl
from jax.experimental.pallas import tpu as pltpu
from jax.sharding import PartitionSpec as P


HEAD_DIM = 128
NORM_EPS = 1e-5
ROPE_BASE = 10000.0
LOG2E = 1.4426950408889634
BF16 = jnp.bfloat16
F32 = jnp.float32
ANY = pl.BlockSpec(memory_space=pl.ANY)
VMEM_LIMIT = 62 * 1024 * 1024


def cost(flops, bytes_accessed):
    return pl.CostEstimate(flops=int(flops), bytes_accessed=int(bytes_accessed), transcendentals=0)


def params(n_axes=1):
    return pltpu.CompilerParams(dimension_semantics=("arbitrary",) * n_axes, vmem_limit_bytes=VMEM_LIMIT)


def norm_kernel(hidden_ref, gain_ref, out_ref):
    h = hidden_ref[0].astype(F32)
    inv = lax.rsqrt(jnp.mean(h * h, axis=-1, keepdims=True) + NORM_EPS)
    out_ref[...] = (h * inv * gain_ref[...].astype(F32)).astype(BF16)


def norm_row(hidden, gain2d, row):
    _, toks, width = hidden.shape
    blk = toks // 2
    return pl.pallas_call(
        norm_kernel,
        grid=(2,),
        out_shape=jax.ShapeDtypeStruct((toks, width), BF16),
        in_specs=[pl.BlockSpec((1, blk, width), lambda i: (row, i, 0)), pl.BlockSpec((1, width), lambda i: (0, 0))],
        out_specs=pl.BlockSpec((blk, width), lambda i: (i, 0)),
        compiler_params=params(),
        cost_estimate=cost(2e9, 4 * toks * width),
    )(hidden, gain2d)


def rotate(vals, cos_tab, sin_tab):
    lanes = vals.shape[-1]
    lane = lax.broadcasted_iota(jnp.int32, vals.shape, 1)
    swapped = jnp.where(lane % 2 == 0, pltpu.roll(vals, lanes - 1, 1), pltpu.roll(vals, 1, 1))
    return vals * cos_tab + swapped * sin_tab


K_PARTS = 4


def split_pieces(pieces):
    return [p if not isinstance(p, tuple) else p[0] for p in pieces], tuple(None if not isinstance(p, tuple) else p[1] for p in pieces)


def row_refs(refs, picks):
    return [r if pick is None else r.at[pick] for r, pick in zip(refs, picks)]


def here(chips):
    me = lax.axis_index('tp')
    return lax.rem(me // 2, chips), lax.rem(me, 2)


def project_kernel(chips, steps, picks, turns, flipped, own_tabs, has_tabs, *refs):
    n, n_w = len(steps), len(turns)
    chip, core = here(chips)
    blocks = [lax.rem(chip + step, chips) for step in steps]
    pieces = row_refs(refs[:4 * n], picks)
    weights = refs[4 * n:4 * n + n_w]
    tabs = refs[4 * n + n_w:4 * n + n_w + 2] if has_tabs else ()
    lhs, wbuf, acc, tab, stage, lhs_sem, w_sem, tab_sem, out_sem = refs[-9:]
    outs = refs[-9 - n_w:-9]
    toks = pieces[0].shape[0]
    part = lhs.shape[2]
    cols = outs[0].shape[2]
    chunk = 2 * toks

    def fetch(k):
        at = pl.ds(pl.multiple_of(k * part, part), part)
        for w in range(n_w):
            if flipped:
                yield pltpu.make_async_copy(weights[w].at[:, at], wbuf.at[k, pl.ds(w * cols, cols), :], w_sem.at[k, w])
            else:
                yield pltpu.make_async_copy(weights[w].at[at, :], wbuf.at[k, :, pl.ds(w * cols, cols)], w_sem.at[k, w])
        for idx, piece in enumerate(pieces):
            c, rel_core, row = idx // 4, (idx % 4) // 2, idx % 2
            slot = 4 * c + 2 * row + lax.rem(core + rel_core, 2)
            yield pltpu.make_async_copy(
                piece.at[:, at], lhs.at[k, pl.ds(pl.multiple_of(slot * toks, toks), toks), :], lhs_sem.at[k, idx])

    def fetch_tabs():
        for c in range(n):
            first = 0 if own_tabs else pl.multiple_of(blocks[c] * chunk, chunk)
            for t, ref in enumerate(tabs):
                yield pltpu.make_async_copy(ref.at[:, pl.ds(first, chunk), :], tab.at[c, t], tab_sem.at[c, t])

    for k in range(K_PARTS):
        for copy in fetch(k):
            copy.start()
    for copy in fetch_tabs():
        copy.start()
    acc[...] = jnp.zeros_like(acc)

    def body(k, carry):
        for copy in fetch(k):
            copy.wait()

        if flipped:
            acc[...] += lax.dot_general(lhs[k], wbuf[k], (((1,), (1,)), ((), ())), preferred_element_type=F32)
            return carry

        def one(c, carry):
            at = pl.ds(pl.multiple_of(c * 4 * toks, 4 * toks), 4 * toks)
            acc[at, :] += jnp.dot(lhs[k, at, :], wbuf[k], preferred_element_type=F32)
            return carry

        return lax.fori_loop(0, n, one, carry) if n > 1 else one(0, carry)

    lax.fori_loop(0, K_PARTS, body, 0)
    for copy in fetch_tabs():
        copy.wait()

    def give(w, c):
        at = pl.ds(pl.multiple_of(blocks[c] * chunk, chunk), chunk)
        return pltpu.make_async_copy(stage.at[w, c], outs[w].at[:, at, :], out_sem.at[w, c])

    for w, turn in enumerate(turns):
        def finish(idx, carry, w=w, turn=turn):
            c, row = idx // 2, lax.rem(idx, 2)
            at = pl.ds(pl.multiple_of(idx * chunk, chunk), chunk)
            for head in range(cols // HEAD_DIM):
                lanes = slice(head * HEAD_DIM, (head + 1) * HEAD_DIM)
                val = acc[at, w * cols + head * HEAD_DIM:w * cols + (head + 1) * HEAD_DIM]
                if turn:
                    val = rotate(val, tab[c, 0, row], tab[c, 1, row])
                stage[w, c, row, :, lanes] = val.astype(BF16)
            return carry

        lax.fori_loop(0, 2 * n, finish, 0)
        for c in range(n):
            give(w, c).start()
    for w in range(n_w):
        for c in range(n):
            give(w, c).wait()


def project(chips, steps, chunks, weights, turns, tabs, bufs, seq, flipped=False, own_tabs=False):
    pieces, picks = split_pieces([p for c in chunks for p in c])
    toks, width = pieces[0].shape[-2:]
    cols = weights[0].shape[0 if flipped else 1]
    n, n_w = len(chunks), len(weights)
    part = width // K_PARTS
    extra = list(bufs) if bufs is not None else []
    n_in = len(pieces) + n_w + len(tabs)
    w_shape = (K_PARTS, n_w * cols, part) if flipped else (K_PARTS, part, n_w * cols)
    return pl.pallas_call(
        functools.partial(project_kernel, chips, steps, picks, turns, flipped, own_tabs, bool(tabs)),
        grid_spec=pltpu.PrefetchScalarGridSpec(
            num_scalar_prefetch=0,
            grid=(1,),
            in_specs=[ANY] * (n_in + len(extra)),
            out_specs=[ANY] * n_w,
            scratch_shapes=[
                pltpu.VMEM((K_PARTS, 4 * n * toks, part), BF16), pltpu.VMEM(w_shape, BF16),
                pltpu.VMEM((4 * n * toks, n_w * cols), F32), pltpu.VMEM((n, 2, 2, 2 * toks, HEAD_DIM), F32),
                pltpu.VMEM((n_w, n, 2, 2 * toks, cols), BF16),
                pltpu.SemaphoreType.DMA((K_PARTS, 4 * n)), pltpu.SemaphoreType.DMA((K_PARTS, n_w)),
                pltpu.SemaphoreType.DMA((n, 2)), pltpu.SemaphoreType.DMA((n_w, n))],
        ),
        out_shape=[jax.ShapeDtypeStruct((2, seq, cols), BF16)] * n_w,
        input_output_aliases={n_in + i: i for i in range(len(extra))},
        compiler_params=params(),
        cost_estimate=cost(2 * 4 * toks * n * width * cols * n_w, 16e6),
    )(*pieces, *weights, *tabs, *extra)


def weight_grad_kernel(n_pieces, picks, n_acts, acts_left, *refs):
    pieces, acts = row_refs(refs[:n_pieces], picks), refs[n_pieces:n_pieces + n_acts]
    if acts_left:
        *refs, act_t = refs
    act, tiles, piece_sem, act_sem = refs[-4:]
    n_out = 1 if acts_left else n_acts // 2
    outs = refs[-4 - n_out:-4]
    step, steps = pl.program_id(0), pl.num_programs(0)
    toks = pieces[0].shape[0]
    cols = acts[0].shape[2]
    seq = 2 * acts[0].shape[1]
    tile = tiles.shape[2]

    def fetch(at, slot):
        for idx, piece in enumerate(pieces):
            yield pltpu.make_async_copy(
                piece.at[:, pl.ds(pl.multiple_of(at * tile, tile), tile)],
                tiles.at[slot, pl.ds(idx * toks, toks), :], piece_sem.at[slot, idx])

    def fetch_acts():
        for idx, a in enumerate(acts):
            for row in range(2):
                yield pltpu.make_async_copy(
                    a.at[row], act.at[pl.ds((2 * row + idx % 2) * seq // 2, seq // 2), pl.ds(idx // 2 * cols, cols)],
                    act_sem.at[2 * idx + row])

    slot = lax.rem(step, 2)

    @pl.when(step == 0)
    def _():
        for c in fetch_acts():
            c.start()
        for c in fetch(0, 0):
            c.start()
        for c in fetch_acts():
            c.wait()
        if acts_left:
            act_t[...] = act[...].T

    @pl.when(step + 1 < steps)
    def _():
        for c in fetch(step + 1, 1 - slot):
            c.start()

    for c in fetch(step, slot):
        c.wait()
    dims = (((0,), (0,)), ((), ()))
    if acts_left:
        outs[0][...] = jnp.dot(act_t[...], tiles[slot], preferred_element_type=F32)
    else:
        res = lax.dot_general(tiles[slot], act[...], dims, preferred_element_type=F32)
        for idx, o in enumerate(outs):
            o[...] = res[:, idx * cols:(idx + 1) * cols]


def weight_grad(pieces, acts, acts_left):
    pieces, picks = split_pieces(pieces)
    _, width = pieces[0].shape[-2:]
    seq, cols = 2 * acts[0].shape[1], acts[0].shape[2]
    tile = 512
    n_acts = len(acts) // 2
    steps = width // tile
    if acts_left:
        out_shape = [jax.ShapeDtypeStruct((cols, width), F32)]
        out_specs = [pl.BlockSpec((cols, tile), lambda i: (0, i))]
    else:
        out_shape = [jax.ShapeDtypeStruct((width, cols), F32)] * n_acts
        out_specs = [pl.BlockSpec((tile, cols), lambda i: (i, 0))] * n_acts
    return pl.pallas_call(
        functools.partial(weight_grad_kernel, len(pieces), picks, len(acts), acts_left),
        grid=(steps,),
        in_specs=[ANY] * (len(pieces) + len(acts)),
        out_specs=out_specs,
        out_shape=out_shape,
        scratch_shapes=[pltpu.VMEM((2 * seq, n_acts * cols), BF16), pltpu.VMEM((2, 2 * seq, tile), BF16),
                        pltpu.SemaphoreType.DMA((2, len(pieces))), pltpu.SemaphoreType.DMA((4 * n_acts,))]
                       + ([pltpu.VMEM((cols, 2 * seq), BF16)] if acts_left else []),
        compiler_params=params(),
        cost_estimate=cost(2 * 2 * seq * steps * tile * cols * n_acts, 40e6),
    )(*pieces, *acts)


def store_rel(halves, vals, block, chips):
    half = vals.shape[0] // 2
    chip, mine = here(chips)
    rel = lax.rem(block - chip + chips, chips)
    for core in range(2):
        halves[lax.rem(core + mine, 2), pl.ds(pl.multiple_of(rel * half, half), half), :] = vals[core * half:(core + 1) * half]


def probs_t(k_ref, q_blk, pos_ref, block, size):
    n = (block + 1) * size
    s_t = lax.dot_general(k_ref[0, :n, :], q_blk, (((1,), (1,)), ((), ())), preferred_element_type=F32)
    key = lax.broadcasted_iota(jnp.int32, (n, size), 0)
    query = lax.broadcasted_iota(jnp.int32, (1, size), 1) + block * size
    first = query - pos_ref[0, :, block * size:n]
    old = n - size
    near = jnp.where((key[old:] >= first) & (key[old:] <= query), s_t[old:], -1e30)
    s_t = jnp.concatenate([jnp.where(key[:old] >= first, s_t[:old], -1e30), near], axis=0) if old else near
    top = jnp.max(s_t, axis=0, keepdims=True)
    e = jnp.exp2((s_t - top) * (LOG2E * HEAD_DIM ** -0.5))
    return e * (1.0 / jnp.sum(e, axis=0, keepdims=True))


def attn_fwd_kernel(chips, q_ref, k_ref, v_ref, pos_ref, o_mine, o_theirs, o_halves):
    seq = q_ref.shape[1]
    size = seq // chips
    v_t = v_ref[0].T
    for block in range(chips):
        n = (block + 1) * size
        p_t = probs_t(k_ref, q_ref[0, block * size:n, :], pos_ref, block, size).astype(BF16)
        o_t = jnp.dot(v_t[:, :n], p_t, preferred_element_type=F32)
        store_rel(o_halves, o_t.T.astype(BF16), block, chips)
    o_mine[0] = o_halves[0]
    o_theirs[0] = o_halves[1]


def attn_bwd_kernel(chips, q_ref, k_ref, v_ref, g_ref, pos_ref, cos_ref, sin_ref, *refs):
    outs, (dk_acc, dv_acc, dq_halves, dk_halves, dv_halves) = refs[:6], refs[6:]
    seq = q_ref.shape[1]
    size = seq // chips
    k_t = k_ref[0].T
    for block in range(chips - 1, -1, -1):
        n = (block + 1) * size
        mine = slice(block * size, n)
        q_blk = q_ref[0, mine, :]
        g_blk = g_ref[0, mine, :]
        p_t = probs_t(k_ref, q_blk, pos_ref, block, size)
        dp_t = lax.dot_general(v_ref[0, :n, :], g_blk, (((1,), (1,)), ((), ())), preferred_element_type=F32)
        row_dot = jnp.sum(p_t * dp_t, axis=0, keepdims=True)
        ds_t = (p_t * (dp_t - row_dot) * (HEAD_DIM ** -0.5)).astype(BF16)
        dv_new = jnp.dot(p_t.astype(BF16), g_blk, preferred_element_type=F32)
        dk_new = jnp.dot(ds_t, q_blk, preferred_element_type=F32)
        if block == chips - 1:
            dv_acc[...] = dv_new
            dk_acc[...] = dk_new
        else:
            dv_acc[:n, :] += dv_new
            dk_acc[:n, :] += dk_new
        dq = jnp.dot(k_t[:, :n], ds_t, preferred_element_type=F32).T
        dq = rotate(dq, cos_ref[0, mine, :], -sin_ref[0, mine, :])
        store_rel(dq_halves, dq.astype(BF16), block, chips)
    for block in range(chips):
        mine = slice(block * size, (block + 1) * size)
        dk = rotate(dk_acc[mine, :], cos_ref[0, mine, :], -sin_ref[0, mine, :])
        store_rel(dk_halves, dk.astype(BF16), block, chips)
        store_rel(dv_halves, dv_acc[mine, :].astype(BF16), block, chips)
    for idx, halves in enumerate((dq_halves, dk_halves, dv_halves)):
        outs[2 * idx][0] = halves[0]
        outs[2 * idx + 1][0] = halves[1]


def attention_specs(seq):
    head = pl.BlockSpec((1, seq, HEAD_DIM), lambda b, h: (b, 0, h))
    half = pl.BlockSpec((1, seq // 2, HEAD_DIM), lambda b, h: (b, 0, h))
    pos = pl.BlockSpec((1, 1, seq), lambda b, h: (b, 0, 0))
    tab = pl.BlockSpec((1, seq, HEAD_DIM), lambda b, h: (b, 0, 0))
    return head, half, pos, tab


def attention_fwd(chips, q, k, v, pos):
    rows, seq, cols = q.shape
    head, half, pos_spec, _ = attention_specs(seq)
    return pl.pallas_call(
        functools.partial(attn_fwd_kernel, chips),
        grid=(rows, cols // HEAD_DIM),
        in_specs=[head, head, head, pos_spec], out_specs=[half] * 2,
        scratch_shapes=[pltpu.VMEM((2, seq // 2, HEAD_DIM), BF16)],
        out_shape=[jax.ShapeDtypeStruct((rows, seq // 2, cols), BF16)] * 2,
        compiler_params=params(2),
        cost_estimate=cost(20e9, 8e6),
    )(q, k, v, pos)


def attention_bwd(chips, q, k, v, grad_o, pos, cos_tab, sin_tab):
    rows, seq, cols = q.shape
    head, half, pos_spec, tab = attention_specs(seq)
    return pl.pallas_call(
        functools.partial(attn_bwd_kernel, chips),
        grid=(rows, cols // HEAD_DIM),
        in_specs=[head, head, head, head, pos_spec, tab, tab], out_specs=[half] * 6,
        scratch_shapes=[pltpu.VMEM((seq, HEAD_DIM), F32)] * 2 + [pltpu.VMEM((2, seq // 2, HEAD_DIM), BF16)] * 3,
        out_shape=[jax.ShapeDtypeStruct((rows, seq // 2, cols), BF16)] * 6,
        compiler_params=params(2),
        cost_estimate=cost(40e9, 16e6),
    )(q, k, v, grad_o, pos, cos_tab, sin_tab)


def share_kernel(n_pairs, n_dest, flipped, *refs):
    lhs = refs[:n_pairs * n_dest]
    weights = refs[n_pairs * n_dest:n_pairs * n_dest + n_pairs]
    outs = refs[-2 * n_dest:]
    acc = None
    for pair in range(n_pairs):
        parts = [lhs[dest * n_pairs + pair][...] for dest in range(n_dest)]
        a = jnp.concatenate([p.reshape(p.shape[0] * p.shape[1], p.shape[2]) for p in parts], axis=0)
        term = lax.dot_general(a, weights[pair][...], (((1,), (1 if flipped else 0,)), ((), ())), preferred_element_type=F32)
        acc = term if acc is None else acc + term
    half = acc.shape[0] // (2 * n_dest)
    for idx, o in enumerate(outs):
        o[...] = acc[idx * half:(idx + 1) * half].astype(o.dtype)


def shares(toks, mine, partner, weights, flipped, dests, dtypes, deps=()):
    cols = mine[0].shape[2]
    width = weights[0].shape[0 if flipped else 1]
    tile = 512 if len(dests) > 1 and flipped else 1024
    n_pairs = len(mine) + len(partner)
    in_specs, operands = [], []
    for d in dests:
        for a in list(mine) + list(partner):
            in_specs.append(pl.BlockSpec((2, toks, cols), lambda j, d=d: (0, d, 0)))
            operands.append(a)
    w_spec = pl.BlockSpec((tile, cols), lambda j: (j, 0)) if flipped else pl.BlockSpec((cols, tile), lambda j: (0, j))
    in_specs += [w_spec] * len(weights) + [ANY] * len(deps)
    n_dest = len(dests)
    return pl.pallas_call(
        functools.partial(share_kernel, n_pairs, n_dest, flipped),
        grid=(width // tile,),
        out_shape=[jax.ShapeDtypeStruct((toks, width), dt) for dt in dtypes],
        in_specs=in_specs,
        out_specs=[pl.BlockSpec((toks, tile), lambda j: (0, j))] * (2 * n_dest),
        compiler_params=params(),
        cost_estimate=cost(2 * 2 * toks * n_dest * n_pairs * cols * width, n_pairs * cols * width * 2),
    )(*operands, *weights, *deps)


SUB_ROWS = 16


def by_rows(block, fn):
    def body(i, carry):
        fn(pl.ds(pl.multiple_of(i * SUB_ROWS, SUB_ROWS), SUB_ROWS))
        return carry

    lax.fori_loop(0, block // SUB_ROWS, body, 0)


def tail_kernel(h_ref, g_ref, gain_ref, own0, own1, left0, left1, right0, right1, out_ref, gg_ref, gg_acc):
    step = pl.program_id(0)

    @pl.when(step == 0)
    def _():
        gg_acc[...] = jnp.zeros_like(gg_acc)

    def finish(own, left, right):
        def some(at):
            h = h_ref[0, at, :].astype(F32)
            inv = lax.rsqrt(jnp.mean(h * h, axis=-1, keepdims=True) + NORM_EPS)
            grad = own[at, :] + left[at, :].astype(F32) + right[at, :].astype(F32)
            unit = grad * (h * inv)
            gg_acc[...] += unit[:8] + unit[8:]
            scaled = grad * gain_ref[...].astype(F32)
            mean_term = jnp.mean(scaled * h, axis=-1, keepdims=True)
            out_ref[0, at, :] = (g_ref[0, at, :].astype(F32) + inv * scaled - h * (inv * inv * inv) * mean_term).astype(BF16)

        by_rows(h_ref.shape[1], some)

    @pl.when(step < 2)
    def _():
        finish(own0, left0, right0)

    @pl.when(step >= 2)
    def _():
        finish(own1, left1, right1)

    @pl.when(step == 3)
    def _():
        gg_ref[...] = jnp.sum(gg_acc[...], axis=0, keepdims=True)


def row_specs(toks, width):
    blk = toks // 2
    whole = pl.BlockSpec((1, blk, width), lambda i: (i // 2, i % 2, 0))
    return whole, [pl.BlockSpec((blk, width), lambda i, r=r: (jnp.clip(i - 2 * r, 0, 1), 0)) for r in range(2)]


def finish_norm(hidden, grad_out, gain2d, own, left, right):
    _, toks, width = hidden.shape
    whole, per_row = row_specs(toks, width)
    one = pl.BlockSpec((1, width), lambda i: (0, 0))
    return pl.pallas_call(
        tail_kernel,
        grid=(4,),
        out_shape=[jax.ShapeDtypeStruct(hidden.shape, BF16), jax.ShapeDtypeStruct((1, width), F32)],
        in_specs=[whole, whole, one] + per_row * 3,
        out_specs=[whole, one],
        scratch_shapes=[pltpu.VMEM((8, width), F32)],
        compiler_params=params(),
        cost_estimate=cost(4e9, 14e6),
    )(hidden, grad_out, gain2d, *own, *left, *right)


def residual_kernel(h_ref, own, left, right, *rest):
    out_ref = rest[-1]

    def some(at):
        attn = (own[at, :] + left[at, :].astype(F32) + right[at, :].astype(F32)).astype(BF16)
        out_ref[0, at, :] = (h_ref[0, at, :].astype(F32) + attn.astype(F32)).astype(BF16)

    by_rows(h_ref.shape[1], some)


def finish_residual(hidden, row, own, left, right, buf=()):
    _, toks, width = hidden.shape
    blk = toks // 2
    whole = pl.BlockSpec((1, blk, width), lambda i: (row, i, 0))
    part = pl.BlockSpec((blk, width), lambda i: (i, 0))
    return pl.pallas_call(
        residual_kernel,
        grid=(2,),
        out_shape=jax.ShapeDtypeStruct(hidden.shape, BF16),
        in_specs=[whole, part, part, part] + [ANY] * len(buf),
        out_specs=whole,
        input_output_aliases={4: 0} if buf else {},
        compiler_params=params(),
        cost_estimate=cost(1e9, 6e6),
    )(hidden, own, left, right, *buf)


def relay_kernel(a0, a1, b0, b1, o0, o1):
    def some(at):
        o0[at, :] = (a0[at, :] + b0[at, :].astype(F32)).astype(BF16)
        o1[at, :] = (a1[at, :] + b1[at, :].astype(F32)).astype(BF16)

    by_rows(a0.shape[0], some)


def relay(own, received):
    toks, width = own[0].shape
    spec = pl.BlockSpec((toks // 4, width), lambda i: (i, 0))
    return pl.pallas_call(
        relay_kernel,
        grid=(4,),
        out_shape=[jax.ShapeDtypeStruct((toks, width), BF16)] * 2,
        in_specs=[spec] * 4,
        out_specs=[spec] * 2,
        compiler_params=params(),
        cost_estimate=cost(1e9, 8e6),
    )(*own, *received)


def solution(mesh):
    tp_size = mesh.shape['tp']
    chips = tp_size // 2

    def move(value, chip_step):
        return lax.ppermute(value, 'tp', [(2 * x + c, 2 * ((x + chip_step) % chips) + c) for x in range(chips) for c in range(2)])

    def swap(value):
        return lax.ppermute(value, 'tp', [(2 * x + c, 2 * x + 1 - c) for x in range(chips) for c in range(2)])

    def device_step(hidden, positions, doc_ids, norm_gain, w_query, w_key, w_value, w_out, grad_out):
        rows, toks, width = hidden.shape
        seq = toks * tp_size
        me = lax.axis_index('tp')
        chip, core = me // 2, me % 2

        def both_cores(own, other):
            return jnp.where(core == 0, jnp.concatenate([own, other], axis=-1), jnp.concatenate([other, own], axis=-1))

        def tables(pos):
            inv_freq = ROPE_BASE ** (-(2 * (jnp.arange(HEAD_DIM) // 2)).astype(F32) / HEAD_DIM)
            angles = pos.astype(F32)[:, :, None] * inv_freq
            return jnp.cos(angles), jnp.where(jnp.arange(HEAD_DIM) % 2 == 0, -1.0, 1.0) * jnp.sin(angles)

        in_w, turns = [w_query, w_key, w_value], (True, True, False)

        gain2d = norm_gain.reshape(1, width)
        own_pos = both_cores(positions, swap(positions))

        def both_rows(a):
            return (a, 0), (a, 1)

        g0, g1 = grad_out[0], grad_out[1]
        grad_pieces = {0: (*both_rows(grad_out), *both_rows(swap(grad_out)))}
        buf = project(chips, (0,), [grad_pieces[0]], [w_out], (False,), (), None, seq, flipped=True)
        n0 = norm_row(hidden, gain2d, 0)
        n1 = norm_row(hidden, gain2d, 1)
        left0, right1 = move(n0, 1), move(n1, -1)
        pieces = {0: (n0, n1, swap(n0), swap(n1))}
        far_pos = [move(own_pos, -1), move(own_pos, 2), move(own_pos, 1)]
        left1, right0 = move(n1, 1), move(n0, -1)
        other_w = [swap(w) for w in (w_out, w_query, w_key, w_value)]
        qkv = project(chips, (0,), [pieces[0]], in_w, turns, tables(own_pos), None, seq, own_tabs=True)
        *far_pos, q0 = lax.optimization_barrier((*far_pos, qkv[0]))
        qkv = [q0, *qkv[1:]]
        pos_rel = jnp.stack([own_pos, *far_pos], axis=1)
        far0, far1 = move(left0, 1), move(right1, -1)

        g_left0, g_right1 = move(g0, 1), move(g1, -1)
        g_left1, g_right0 = move(g1, 1), move(g0, -1)

        twice = jnp.concatenate([pos_rel, pos_rel], axis=1)
        pos_full = lax.dynamic_slice_in_dim(twice, (chips - chip) % chips, chips, axis=1).reshape(rows, seq)
        pos3 = pos_full.reshape(rows, 1, seq)
        tabs = cos_tab, sin_tab = tables(pos_full)
        pieces[3] = (left0, left1, swap(left0), swap(left1))
        pieces[1] = (right0, right1, swap(right0), swap(right1))
        qkv = project(chips, (1, 3), [pieces[1], pieces[3]], in_w, turns, tabs, qkv, seq)
        pieces[2] = (far0, far1, swap(far0), swap(far1))
        q, k, v = project(chips, (2,), [pieces[2]], in_w, turns, tabs, qkv, seq)
        w_out_both = [w_out, other_w[0]]
        in_both = in_w + other_w[1:]
        g_far0, g_far1 = move(g_left0, 1), move(g_right1, -1)
        grad_pieces[3] = (g_left0, g_left1, swap(g_left0), swap(g_left1))
        grad_pieces[1] = (g_right0, g_right1, swap(g_right0), swap(g_right1))
        grad_pieces[2] = (g_far0, g_far1, swap(g_far0), swap(g_far1))
        o_mine, o_theirs = attention_fwd(chips, q, k, v, pos3)

        share_o = functools.partial(shares, toks, [o_mine], [swap(o_theirs)], w_out_both, False)
        o_two0, o_two1, o_one0, o_one1, o_three0, o_three1, *o_own = share_o(
            (2, 1, 3, 0), (BF16, BF16, F32, BF16, BF16, F32, F32, F32))
        o_relay = move(o_two0, 1), move(o_two1, -1)
        o_left1, o_right0 = move(o_one1, 1), move(o_three0, -1)

        (buf,) = project(chips, (1, 3, 2), [grad_pieces[s] for s in (1, 3, 2)], [w_out], (False,), (), buf, seq, flipped=True)
        grads = attention_bwd(chips, q, k, v, buf, pos3, cos_tab, sin_tab)
        o_one0, o_three1 = relay((o_one0, o_three1), o_relay)
        o_left0, o_right1 = move(o_one0, 1), move(o_three1, -1)

        def whole(pieces):
            return [pieces[s][2 * c + r] for r in range(rows) for c in range(2) for s in range(chips)]

        share_g = functools.partial(shares, toks, grads[::2], [swap(a) for a in grads[1::2]], in_both, True)
        g_two = share_g((2,), (BF16, BF16))
        g_relay = move(g_two[0], 1), move(g_two[1], -1)
        g_one0, g_one1, g_three0, g_three1, g_own0, g_own1 = share_g((1, 3, 0), (F32, BF16, BF16, F32, F32, F32))
        d_left1, d_right0 = move(g_one1, 1), move(g_three0, -1)

        (grad_w_out,) = weight_grad(whole(grad_pieces), [o_mine, o_theirs], True)
        g_one0, g_three1 = relay((g_one0, g_three1), g_relay)
        d_left0, d_right1 = move(g_one0, 1), move(g_three1, -1)
        grad_wq, grad_wk, grad_wv = weight_grad(whole(pieces), grads, False)
        attn_out = finish_residual(hidden, 0, o_own[0], o_left0, o_right0)
        attn_out = finish_residual(hidden, 1, o_own[1], o_left1, o_right1, (attn_out,))

        grad_hidden, grad_gain = finish_norm(hidden, grad_out, gain2d, (g_own0, g_own1), (d_left0, d_left1), (d_right0, d_right1))
        grad_gain = grad_gain.reshape(width)
        grad_gain = grad_gain + swap(grad_gain)
        for turn in (0, 1):
            pairs = [(x, x ^ 1) if turn == 0 else (x, chips - 1 - x) for x in range(chips)]
            grad_gain = grad_gain + lax.ppermute(grad_gain, 'tp', [(2 * a + c, 2 * b + c) for a, b in pairs for c in range(2)])
        return (attn_out, grad_hidden, grad_gain, grad_wq, grad_wk, grad_wv, grad_w_out)

    row_spec = P('dp', 'tp', None)
    tok_spec = P('dp', 'tp')
    col_spec = P(None, 'tp')
    return jax.shard_map(
        device_step, mesh=mesh,
        in_specs=(row_spec, tok_spec, tok_spec, P(), col_spec, col_spec, col_spec, P('tp', None), row_spec),
        out_specs=(row_spec, row_spec, P('dp'), P('dp', 'tp'), P('dp', 'tp'), P('dp', 'tp'), P(('dp', 'tp'), None)),
        check_vma=False)
```
